32 devices in a mesh: lat: 4 (over x, core), lon: 8 (over z, y).
Axes of the slice: x: 2, y: 2, z: 4, core: 2. Of those that a mesh axis runs over, the one named last changes fastest.
Arguments:
- prediction_fields: float32 [4, 69, 360, 512], P(None, None, 'lon', 'lat'), may hold values from -16 to 16
- verifying_state: float32 [69, 360, 512], P(None, 'lon', 'lat'), may hold values from -16 to 16
- normal_state: float32 [69, 360, 512], P(None, 'lon', 'lat'), may hold values from -16 to 16
- evaluated_point_flag: int32 [360, 512], P('lon', 'lat'), may hold values 0 or 1
- parallels_each_strip: int32 [4], replicated, may hold values from 1 to 128, 361 in all
Outputs:
- parallel_quadratic_error: float32 [4, 69, 512], P(None, None, 'lat')
- parallel_systematic_error: float32 [4, 69, 512], P(None, None, 'lat')
- parallel_pattern_skill: float32 [4, 69, 512], P(None, None, 'lat')
- rmse: float32 [4, 69], replicated
- systematic_error: float32 [4, 69], replicated
- pattern_skill: float32 [4, 69], replicated
The draws below stay inside these ranges and needn't reach their ends.
Inputs may be any that keep to these rules, and one draw needn't show every extreme that they name: `parallels_each_strip`: they sum to 361, and some band holds exactly 128 rows.
All inputs are finite; a program needn't handle non-finite values.
Results may differ from the reference program's by a relative error of at most 0.00002.
Values sent between devices are 32-bit elements.
A program may use at most 64 MiB of HBM per device.

```python
import math
import jax
import jax.numpy as jnp
import numpy as np
from jax import lax

VARS = 69
LEADS = 4
LAT_CAP = 128
LAT_BANDS = 4
NLAT = 361
EAST_WEST_SIZE = 360
LAT_BUF = 512


def common_fields(key):
    subkeys = jax.random.split(jax.random.fold_in(key, 4242), 8)
    climate = jax.random.normal(subkeys[0], (VARS, EAST_WEST_SIZE, LAT_BUF), jnp.float32)
    amplitude = jnp.exp(jax.random.uniform(subkeys[1], (VARS, 1, LAT_BUF), jnp.float32, jnp.log(0.5), jnp.log(2.0)))
    anomaly = jax.random.normal(subkeys[2], (VARS, EAST_WEST_SIZE, LAT_BUF), jnp.float32) * amplitude
    observed = climate + anomaly
    skill = jax.random.uniform(subkeys[4], (LEADS, VARS, 1, 1), jnp.float32, 0.3, 0.95)
    noise_scale = jax.random.uniform(subkeys[5], (LEADS, VARS, 1, 1), jnp.float32, 0.6, 1.2)
    drift = jax.random.uniform(subkeys[6], (LEADS, VARS, 1, LAT_BUF), jnp.float32, -0.6, 0.6)
    noise = jax.random.normal(subkeys[7], (LEADS, VARS, EAST_WEST_SIZE, LAT_BUF), jnp.float32)
    predicted = climate[None] + skill * anomaly[None] + noise_scale * amplitude[None] * noise + drift
    return (jnp.clip(predicted, -16.0, 16.0), jnp.clip(observed, -16.0, 16.0), jnp.clip(climate, -16.0, 16.0))


def draw_prediction_fields(key, part):
    return common_fields(key)[0]


def draw_verifying_state(key, part):
    return common_fields(key)[1]


def draw_normal_state(key, part):
    return common_fields(key)[2]


def place_ends(values, own_key, least, top_value):
    extent = values.shape
    index_at = [jax.random.randint(jax.random.fold_in(own_key, axis), (), 0, extent[axis]) for axis in range(len(extent))]
    values = values.at[tuple(index_at)].set(least)
    longest = extent.index(max(extent))
    index_at[longest] = (index_at[longest] + 1) % extent[longest]
    return values.at[tuple(index_at)].set(top_value)


def length_profile(count, total, limit, skew):
    portions = [(1 << 20) // math.isqrt(grade ** skew) + 1 for grade in range(2, count + 1)]
    spare, given = total - limit - (count - 1), [1] * (count - 1)
    while spare > 0:
        free = [i for i in range(count - 1) if given[i] < limit]
        mass, remaining = sum([portions[i] for i in free]), spare
        for i in free:
            extra = min(limit - given[i], max(1, remaining * portions[i] // mass), spare)
            given[i] = given[i] + extra
            spare = spare - extra
    return np.array([limit] + given)


def ragged(own_key, number_of, total, most, slope):
    if number_of == 2:
        one = jax.random.randint(own_key, (), max(1, total - most), min(most, total - 1) + 1)
        return jnp.stack([one, total - one])
    sizes = jnp.asarray(length_profile(number_of, total, most, slope), jnp.int32)
    twos = (number_of - 1) // 2
    donor, taker = sizes[1:1 + 2 * twos:2], sizes[2:2 + 2 * twos:2]
    margin = jnp.minimum(donor - 1, most - taker)
    passed = jax.random.randint(jax.random.fold_in(own_key, 1), (twos,), 0, 1 << 20) % (margin + 1)
    sizes = sizes.at[1:1 + 2 * twos:2].set(donor - passed).at[2:2 + 2 * twos:2].set(taker + passed)
    return sizes[jax.random.permutation(jax.random.fold_in(own_key, 2), number_of)]


def setup_inputs(seed: int = 0) -> dict:
    arg_keys = jax.random.split(jax.random.key(seed), 6)
    return {
        "prediction_fields": draw_prediction_fields(jax.random.fold_in(arg_keys[5], 71), 0),
        "verifying_state": draw_verifying_state(jax.random.fold_in(arg_keys[5], 71), 0),
        "normal_state": draw_normal_state(jax.random.fold_in(arg_keys[5], 71), 0),
        "evaluated_point_flag": place_ends((jax.random.randint(arg_keys[3], (EAST_WEST_SIZE, LAT_BUF), 0, 4) < 3).astype(jnp.int32), jax.random.fold_in(arg_keys[3], 1), 0, 1),
        "parallels_each_strip": ragged(arg_keys[4], LAT_BANDS, NLAT, LAT_CAP, 2).astype(jnp.int32),
    }


minimum_divisor = 0.1

def final_result(error_power_two, prediction_error, paired_anomaly_term, predicted_spread_sum, observed_dispersion, grid_point_tally):
    mean_square = error_power_two / grid_point_tally
    average_error = prediction_error / grid_point_tally
    covariance_sum = paired_anomaly_term / grid_point_tally / jnp.sqrt(jnp.maximum(predicted_spread_sum / grid_point_tally, minimum_divisor) * jnp.maximum(observed_dispersion / grid_point_tally, minimum_divisor))
    return (mean_square, average_error, covariance_sum)

def reference(prediction_fields, verifying_state, normal_state, evaluated_point_flag, parallels_each_strip):
    band_start = jnp.cumsum(parallels_each_strip) - parallels_each_strip
    slot_ids = jnp.arange(LAT_CAP, dtype=jnp.int32)
    global_row = (band_start[:, None] + slot_ids[None, :]).reshape(-1)
    inside_band = (slot_ids[None, :] < parallels_each_strip[:, None]).reshape(-1)
    angles = jnp.pi * jnp.arange(NLAT, dtype=jnp.float32) / (NLAT - 1)
    normalizer = jnp.sum(jnp.sin(angles))
    row_angle = jnp.pi * global_row.astype(jnp.float32) / (NLAT - 1)
    area_factors = jnp.where(inside_band, jnp.sin(row_angle) * NLAT / normalizer, 0.0).astype(jnp.float32)
    retain_filter = evaluated_point_flag.astype(jnp.float32) * inside_band.astype(jnp.float32)[None, :]
    observed_anomaly = verifying_state - normal_state
    observed_dispersion = lax.optimization_barrier(jnp.sum(retain_filter * observed_anomaly * observed_anomaly, axis=1))

    def by_horizon(predicted_step):
        predicted_anomaly = predicted_step - normal_state
        mistake_field = predicted_anomaly - observed_anomaly
        return (lax.optimization_barrier(jnp.sum(retain_filter * mistake_field * mistake_field, axis=1)), lax.optimization_barrier(jnp.sum(retain_filter * mistake_field, axis=1)), lax.optimization_barrier(jnp.sum(retain_filter * predicted_anomaly * observed_anomaly, axis=1)), lax.optimization_barrier(jnp.sum(retain_filter * predicted_anomaly * predicted_anomaly, axis=1)))
    error_power_two, prediction_error, paired_anomaly_term, predicted_spread_sum = lax.map(by_horizon, prediction_fields)
    parallel_quadratic_error, parallel_systematic_error, parallel_pattern_skill = final_result(error_power_two, prediction_error, paired_anomaly_term, predicted_spread_sum, observed_dispersion[None], EAST_WEST_SIZE)
    grid_points = NLAT * EAST_WEST_SIZE
    quadratic_error_total, systematic_error, pattern_skill = final_result(lax.optimization_barrier(jnp.sum(error_power_two * area_factors, axis=-1)), lax.optimization_barrier(jnp.sum(prediction_error * area_factors, axis=-1)), lax.optimization_barrier(jnp.sum(paired_anomaly_term * area_factors, axis=-1)), lax.optimization_barrier(jnp.sum(predicted_spread_sum * area_factors, axis=-1)), lax.optimization_barrier(jnp.sum(observed_dispersion * area_factors, axis=-1))[None], grid_points)
    rmse = jnp.sqrt(jnp.maximum(quadratic_error_total, minimum_divisor))
    return (parallel_quadratic_error, parallel_systematic_error, parallel_pattern_skill, rmse, systematic_error, pattern_skill)
```

```python
import functools
import math

import jax
import jax.numpy as jnp
from jax import lax
from jax.experimental import pallas as pl
from jax.experimental.pallas import tpu as pltpu
from jax.sharding import PartitionSpec as P

MEAN_ROWS = 90
FLOOR = 0.1
MESH = pl.DeviceIdType.MESH


def cosine(y):
    y2 = y * y
    terms = [(-1) ** k / math.factorial(2 * k) for k in range(9)]
    total = jnp.full_like(y, terms[-1])
    for term in terms[-2::-1]:
        total = total * y2 + term
    return total


def kernel(n_lat, n_lon, vp, par, pred, ver, norm, flag, o_sq, o_off, o_skill, g_rmse, g_off, g_skill,
           xp, xv, xn, xf, kf, acc, part, one_in, two_out, two_in, tot, truth, fin, g_out, g_in, g_mine, g_all, g_tmp,
           in_sem, flag_sem, one_s, one_r, two_s, two_r, agz_s, agz_r, agy_s, agy_r, lat_s, lat_r, lon_s, lon_r, ):
    leads, nvars, cols, lanes = pred.shape
    pair = 2 if n_lon % 2 == 0 else 1
    outer = n_lon // pair
    band = lax.axis_index("lat")
    me = lax.axis_index("lon")
    a, b = me // pair, me % pair
    ob = (pair - 1) - b
    lv = leads * vp
    rows = 4 * lv + vp

    starts = [min(d * vp, nvars - vp) for d in range(n_lon)]

    def first_var(d):
        return jnp.minimum(d * vp, nvars - vp)

    def other(k):
        return lax.rem(a + k, outer)

    steps = [k for k in range(1, outer)] + [0]
    order = [(k, True) for k in steps] if pair == 2 else []
    order += [(k, False) for k in steps]
    copies = []
    flag_copy = pltpu.make_async_copy(flag, xf, flag_sem)
    flag_copy.start()
    for i, (k, away) in enumerate(order):
        v0 = first_var(other(k) * pair + (ob if away else b))
        group = [
            pltpu.make_async_copy(norm.at[pl.ds(v0, vp)], xn.at[i], in_sem.at[i, 0]),
            pltpu.make_async_copy(ver.at[pl.ds(v0, vp)], xv.at[i], in_sem.at[i, 1]),
            pltpu.make_async_copy(pred.at[:, pl.ds(v0, vp)], xp.at[i], in_sem.at[i, 2]),
        ]
        for c in group:
            c.start()
        copies.append(group)

    barrier = pltpu.get_barrier_semaphore()
    for k in range(1, n_lon):
        pl.semaphore_signal(barrier, inc=1, device_id=(band, lax.rem(me + k, n_lon)), device_id_type=MESH)
    for k in range(1, n_lat):
        pl.semaphore_signal(barrier, inc=1, device_id=(lax.rem(band + k, n_lat), me), device_id_type=MESH)

    first_row = jnp.int32(0)
    filled = jnp.int32(0)
    for i in range(n_lat):
        first_row = first_row + jnp.where(i < band, par[i], 0)
        filled = filled + jnp.where(i == band, par[i], 0)
    total_rows = MEAN_ROWS * n_lat + 1
    slot = lax.broadcasted_iota(jnp.int32, (8, lanes), 1)
    inside = slot < filled
    g = (first_row + slot).astype(jnp.float32)
    normalizer = sum(math.sin(math.pi * r / (total_rows - 1)) for r in range(total_rows))
    angle = (g - 0.5 * (total_rows - 1)) * (math.pi / (total_rows - 1))
    weight = jnp.where(inside, cosine(angle) * (total_rows / normalizer), 0.0)

    flag_copy.wait()
    windows = [8 * i for i in range(cols // 8)]
    if cols % 8:
        windows.append(cols - 8)
    row8 = lax.broadcasted_iota(jnp.int32, (8, lanes), 0)
    for j, w in enumerate(windows):
        keep = jnp.where(inside, xf[w:w + 8, :].astype(jnp.float32), 0.0)
        if cols % 8 and j == len(windows) - 1:
            keep = jnp.where(row8 >= 8 - cols % 8, keep, 0.0)
        kf[j] = keep

    def put(row, value):
        acc[pl.ds(pl.multiple_of(row * 8, 8), 8), :] = value

    def sums(i):
        for c in copies[i]:
            c.wait()

        def one(v, carry):
            nn, tt = [], []
            st = None
            for j, w in enumerate(windows):
                n_ = xn[i, v, w:w + 8, :]
                t_ = kf[j] * (xv[i, v, w:w + 8, :] - n_)
                nn.append(n_)
                tt.append(t_)
                st = t_ * t_ if st is None else st + t_ * t_
            put(4 * lv + v, st)
            for l in range(leads):
                sq = off = pr = sp = None
                for j, w in enumerate(windows):
                    f = kf[j] * (xp[i, l, v, w:w + 8, :] - nn[j])
                    e = f - tt[j]
                    if sq is None:
                        sq, off, pr, sp = e * e, e, f * tt[j], f * f
                    else:
                        sq, off, pr, sp = sq + e * e, off + e, pr + f * tt[j], sp + f * f
                put(l * vp + v, sq)
                put(lv + l * vp + v, off)
                put(2 * lv + l * vp + v, pr)
                put(3 * lv + l * vp + v, sp)
            return carry

        lax.fori_loop(0, vp, one, 0)
        groups = [8 * q for q in range(rows // 8)]
        if rows % 8:
            groups.append(rows - 8)
        for r in groups:
            x = [acc[pl.ds(r * 8 + s, 8, stride=8), :] for s in range(8)]
            part[i, r:r + 8, :] = ((x[0] + x[1]) + (x[2] + x[3])) + ((x[4] + x[5]) + (x[6] + x[7]))

    def remote(src, dst, s, r, device):
        return pltpu.make_async_remote_copy(src_ref=src, dst_ref=dst, send_sem=s, recv_sem=r, device_id=device, device_id_type=MESH)

    partner = (band, a * pair + ob)
    sent = []
    phase_one = {}
    greeted = False
    for i, (k, away) in enumerate(order):
        sums(i)
        if not greeted:
            pl.semaphore_wait(barrier, n_lon - 1 + n_lat - 1)
            greeted = True
        if away:
            c = remote(part.at[i], one_in.at[k], one_s.at[k], one_r.at[k], partner)
            c.start()
            phase_one[k] = c
            sent.append(c)
    phase_two = {}
    base = len(order) - outer
    for q, k in enumerate(steps):
        local = part[base + q]
        if pair == 2:
            phase_one[k].wait_recv()
            local = local + one_in[k]
        if k:
            two_out[k] = local
            c = remote(two_out.at[k], two_in.at[k], two_s.at[k], two_r.at[k], (band, other(k) * pair + b))
            c.start()
            phase_two[k] = c
            sent.append(c)
        else:
            tot[...] = local
    for k in range(1, outer):
        phase_two[k].wait_recv()
    total = tot[...]
    for k in range(1, outer):
        total = total + two_in[k]
    tot[...] = total

    for l in range(leads):
        truth[l * vp:(l + 1) * vp, :] = tot[4 * lv:4 * lv + vp, :]
    blocks = [tot[s * lv:(s + 1) * lv, :] for s in range(4)] + [truth[...]]
    g_out[...] = jnp.zeros_like(g_out)
    for s in range(5):
        d = lax.dot_general(weight, blocks[s], (((1,), (1,)), ((), ())), precision=lax.Precision.HIGHEST,
                            preferred_element_type=jnp.float32)
        g_out[s:s + 1, 0:lv] = d[0:1, :]
    lat_copies = []
    for k in range(1, n_lat):
        c = remote(g_out, g_in.at[k], lat_s.at[k], lat_r.at[k], (lax.rem(band + k, n_lat), me))
        c.start()
        lat_copies.append(c)
        sent.append(c)

    points = float(cols * n_lon)
    square, offset, product, spread = [x / points for x in blocks[:4]]
    fin[me, 0:lv, :] = square
    fin[me, lv:2 * lv, :] = offset
    fin[me, 2 * lv:3 * lv, :] = product / jnp.sqrt(
        jnp.maximum(spread, FLOOR) * jnp.maximum(blocks[4] / points, FLOOR))
    gather_z, gather_y = {}, {}
    if pair == 2:
        c = remote(fin.at[me], fin.at[me], agy_s.at[0], agy_r.at[0], partner)
        c.start()
        gather_y[0] = c
        sent.append(c)
    for k in range(1, outer):
        c = remote(fin.at[me], fin.at[me], agz_s.at[k], agz_r.at[k], (band, other(k) * pair + b))
        c.start()
        gather_z[k] = c
        sent.append(c)

    for c in lat_copies:
        c.wait_recv()
    gs = g_out[...]
    for k in range(1, n_lat):
        gs = gs + g_in[k]
    gs = gs / float(total_rows * cols * n_lon)
    g_mine[...] = gs
    g_all[me, 0:1, :] = jnp.sqrt(jnp.maximum(g_mine[0:1, :], FLOOR))
    g_all[me, 1:2, :] = g_mine[1:2, :]
    g_all[me, 2:3, :] = g_mine[2:3, :] / jnp.sqrt(
        jnp.maximum(g_mine[3:4, :], FLOOR) * jnp.maximum(g_mine[4:5, :], FLOOR))
    g_all[me, 3:8, :] = jnp.zeros((5, g_all.shape[2]), jnp.float32)
    lon_copies = []
    for k in range(1, n_lon):
        c = remote(g_all.at[me], g_all.at[me], lon_s.at[k], lon_r.at[k], (band, lax.rem(me + k, n_lon)))
        c.start()
        lon_copies.append(c)
        sent.append(c)

    for k in sorted(range(1, outer), key=lambda k: min(k, outer - k)):
        gather_z[k].wait_recv()
        if pair == 2:
            source = fin.at[lax.rem(a - k + outer, outer) * pair + b]
            c = remote(source, source, agy_s.at[k], agy_r.at[k], partner)
            c.start()
            gather_y[k] = c
            sent.append(c)
    for c in lon_copies:
        c.wait_recv()
    for d in range(n_lon):
        for l in range(leads):
            g_tmp[l, 0:3, starts[d]:starts[d] + vp] = g_all[d, 0:3, l * vp:(l + 1) * vp]
    for l in range(leads):
        for m, out in enumerate((g_rmse, g_off, g_skill)):
            out[l:l + 1, :] = g_tmp[l, m:m + 1, 0:nvars]
    for k in gather_y:
        gather_y[k].wait_recv()
    for d in range(n_lon):
        for l in range(leads):
            for m, out in enumerate((o_sq, o_off, o_skill)):
                at = m * lv + l * vp
                out[l, starts[d]:starts[d] + vp, :] = fin[d, at:at + vp, :]
    for c in sent:
        c.wait_send()


def local(n_lat, n_lon, pred, ver, norm, flag, par):
    leads, nvars, cols, lanes = pred.shape
    vp = -(-nvars // n_lon)
    outer = n_lon // 2 if n_lon % 2 == 0 else n_lon
    rows = (4 * leads + 1) * vp
    glanes = -(-leads * vp // 128) * 128
    nw = -(-cols // 8)
    f32 = jnp.float32
    dma = pltpu.SemaphoreType.DMA
    vmem = pl.BlockSpec(memory_space=pltpu.VMEM)
    hbm = pl.BlockSpec(memory_space=pl.ANY)
    zonal = jax.ShapeDtypeStruct((leads, nvars, lanes), f32)
    whole = jax.ShapeDtypeStruct((leads, nvars), f32)
    return pl.pallas_call(
        functools.partial(kernel, n_lat, n_lon, vp),
        out_shape=(zonal,) * 3 + (whole,) * 3,
        in_specs=[pl.BlockSpec(memory_space=pltpu.SMEM)] + [hbm] * 4,
        out_specs=(vmem,) * 6,
        scratch_shapes=[
            pltpu.VMEM((n_lon, leads, vp, cols, lanes), f32),
            pltpu.VMEM((n_lon, vp, cols, lanes), f32),
            pltpu.VMEM((n_lon, vp, cols, lanes), f32),
            pltpu.VMEM((cols, lanes), jnp.int32),
            pltpu.VMEM((nw, 8, lanes), f32),
            pltpu.VMEM((rows * 8, lanes), f32),
            pltpu.VMEM((n_lon, rows, lanes), f32),
            pltpu.VMEM((outer, rows, lanes), f32),
            pltpu.VMEM((outer, rows, lanes), f32),
            pltpu.VMEM((outer, rows, lanes), f32),
            pltpu.VMEM((rows, lanes), f32),
            pltpu.VMEM((leads * vp, lanes), f32),
            pltpu.VMEM((n_lon, 3 * leads * vp, lanes), f32),
            pltpu.VMEM((8, glanes), f32),
            pltpu.VMEM((n_lat, 8, glanes), f32),
            pltpu.VMEM((8, glanes), f32),
            pltpu.VMEM((n_lon, 8, glanes), f32),
            pltpu.VMEM((leads, 8, 128 * (-(-nvars // 128))), f32),
            dma((n_lon, 3)), dma,
            dma((outer,)), dma((outer,)), dma((outer,)), dma((outer,)),
            dma((outer,)), dma((outer,)), dma((outer,)), dma((outer,)),
            dma((n_lat,)), dma((n_lat,)), dma((n_lon,)), dma((n_lon,)),
        ],
        compiler_params=pltpu.CompilerParams(collective_id=0, has_side_effects=True),
    )(par, pred, ver, norm, flag)


def solution(mesh):
    n_lat, n_lon = mesh.shape["lat"], mesh.shape["lon"]
    in_specs = (
        P(None, None, "lon", "lat"),
        P(None, "lon", "lat"),
        P(None, "lon", "lat"),
        P("lon", "lat"),
        P(),
    )
    out_specs = (P(None, None, "lat"), P(None, None, "lat"), P(None, None, "lat"), P(), P(), P())
    return jax.shard_map(functools.partial(local, n_lat, n_lon), mesh=mesh, in_specs=in_specs, out_specs=out_specs,
                         check_vma=False)
```

```python
import functools
import math

import jax
import jax.numpy as jnp
from jax import lax
from jax.experimental import pallas as pl
from jax.experimental.pallas import tpu as pltpu
from jax.sharding import PartitionSpec as P

MEAN_ROWS = 90
FLOOR = 0.1
MESH = pl.DeviceIdType.MESH


def cosine(y):
    y2 = y * y
    terms = [(-1) ** k / math.factorial(2 * k) for k in range(9)]
    total = jnp.full_like(y, terms[-1])
    for term in terms[-2::-1]:
        total = total * y2 + term
    return total


def kernel(n_lat, n_lon, vp, par, pred, ver, norm, flag, o_sq, o_off, o_skill, g_rmse, g_off, g_skill,
           xp, xv, xn, xf, kf, spread_t, part, one_in, two_out, two_in, tot, flat, fin, g_out, g_in, g_mine, g_all, g_tmp,
           in_sem, pred_sem, one_s, one_r, two_s, two_r, agz_s, agz_r, agy_s, agy_r, lat_s, lat_r, lon_s, lon_r):
    nvars, cols, leads, lanes = pred.shape
    pair = 2 if n_lon % 2 == 0 else 1
    outer = n_lon // pair
    band = lax.axis_index("lat")
    me = lax.axis_index("lon")
    a, b = me // pair, me % pair
    ob = (pair - 1) - b
    lv = leads * vp
    blocks = part.shape[1]

    starts = [min(d * vp, nvars - vp) for d in range(n_lon)]

    def first_var(d):
        return jnp.minimum(d * vp, nvars - vp)

    def other(k):
        return lax.rem(a + k, outer)

    steps = [k for k in range(1, outer)] + [0]
    order = [(k, True) for k in steps] if pair == 2 else []
    order += [(k, False) for k in steps]
    first = [
        pltpu.make_async_copy(flag, xf, in_sem.at[0]),
        pltpu.make_async_copy(norm, xn, in_sem.at[1]),
        pltpu.make_async_copy(ver, xv, in_sem.at[2]),
    ]
    for c in first:
        c.start()
    chunk_vars, copies = [], []
    for i, (k, away) in enumerate(order):
        v0 = first_var(other(k) * pair + (ob if away else b))
        c = pltpu.make_async_copy(pred.at[pl.ds(v0, vp)], xp.at[i], pred_sem.at[i])
        c.start()
        chunk_vars.append(v0)
        copies.append(c)

    barrier = pltpu.get_barrier_semaphore()
    for k in range(1, n_lon):
        pl.semaphore_signal(barrier, inc=1, device_id=(band, lax.rem(me + k, n_lon)), device_id_type=MESH)
    for k in range(1, n_lat):
        pl.semaphore_signal(barrier, inc=1, device_id=(lax.rem(band + k, n_lat), me), device_id_type=MESH)

    first_row = jnp.int32(0)
    filled = jnp.int32(0)
    for i in range(n_lat):
        first_row = first_row + jnp.where(i < band, par[i], 0)
        filled = filled + jnp.where(i == band, par[i], 0)
    total_rows = MEAN_ROWS * n_lat + 1
    slot = lax.broadcasted_iota(jnp.int32, (8, lanes), 1)
    g = (first_row + slot).astype(jnp.float32)
    normalizer = sum(math.sin(math.pi * r / (total_rows - 1)) for r in range(total_rows))
    angle = (g - 0.5 * (total_rows - 1)) * (math.pi / (total_rows - 1))
    weight = jnp.where(slot < filled, cosine(angle) * (total_rows / normalizer), 0.0)
    if vp % 4:
        for i in range(n_lon):
            part[i, blocks - 1] = jnp.zeros((4, lanes), jnp.float32)

    first[0].wait()
    kf[...] = jnp.where(lax.broadcasted_iota(jnp.int32, (cols, lanes), 1) < filled, xf[...].astype(jnp.float32), 0.0)
    first[1].wait()
    first[2].wait()

    def truth_column(c, total):
        t = kf[pl.ds(c, 1), :] * (xv[c] - xn[c])
        xv[c] = t
        return total + t * t

    spread_t[...] = lax.fori_loop(0, cols, truth_column, jnp.zeros((nvars, lanes), jnp.float32))

    def sums(i):
        copies[i].wait()
        v0 = chunk_vars[i]

        def one(v, carry):
            sq = off = pr = sp = None
            for c in range(cols):
                n_ = xn[c, pl.ds(v0 + v, 1), :]
                t_ = xv[c, pl.ds(v0 + v, 1), :]
                f = kf[c:c + 1, :] * (xp[i, v, c] - n_)
                e = f - t_
                if sq is None:
                    sq, off, pr, sp = e * e, e, f * t_, f * f
                else:
                    sq, off, pr, sp = sq + e * e, off + e, pr + f * t_, sp + f * f
            part[i, v] = sq
            part[i, vp + v] = off
            part[i, 2 * vp + v] = pr
            part[i, 3 * vp + v] = sp
            return carry

        lax.fori_loop(0, vp, one, 0)
        for v in range(vp):
            part[i, 4 * vp + v // 4, v % 4:v % 4 + 1, :] = spread_t[pl.ds(v0 + v, 1), :]

    def remote(src, dst, s, r, device):
        return pltpu.make_async_remote_copy(src_ref=src, dst_ref=dst, send_sem=s, recv_sem=r, device_id=device, device_id_type=MESH)

    partner = (band, a * pair + ob)
    sent = []
    phase_one = {}
    greeted = False
    for i, (k, away) in enumerate(order):
        sums(i)
        if not greeted:
            pl.semaphore_wait(barrier, n_lon - 1 + n_lat - 1)
            greeted = True
        if away:
            c = remote(part.at[i], one_in.at[k], one_s.at[k], one_r.at[k], partner)
            c.start()
            phase_one[k] = c
            sent.append(c)
    phase_two = {}
    base = len(order) - outer
    for q, k in enumerate(steps):
        local = part[base + q]
        if pair == 2:
            phase_one[k].wait_recv()
            local = local + one_in[k]
        if k:
            two_out[k] = local
            c = remote(two_out.at[k], two_in.at[k], two_s.at[k], two_r.at[k], (band, other(k) * pair + b))
            c.start()
            phase_two[k] = c
            sent.append(c)
        else:
            tot[...] = local
    for k in range(1, outer):
        phase_two[k].wait_recv()
    total = tot[...]
    for k in range(1, outer):
        total = total + two_in[k]
    tot[...] = total

    points = 1.0 / float(cols * n_lon)
    for v in range(vp):
        sq, off, pr, sp = [tot[s * vp + v] for s in range(4)]
        tr = jnp.broadcast_to(tot[4 * vp + v // 4, v % 4:v % 4 + 1, :], (leads, lanes))
        for s, x in enumerate((sq, off, pr, sp, tr)):
            flat[s, pl.ds(v, leads, stride=vp), :] = x
    g_out[...] = jnp.zeros_like(g_out)
    for s in range(5):
        d = lax.dot_general(weight, flat[s], (((1,), (1,)), ((), ())), precision=lax.Precision.HIGHEST,
                            preferred_element_type=jnp.float32)
        g_out[s:s + 1, 0:lv] = d[0:1, :]
    lat_copies = []
    for k in range(1, n_lat):
        c = remote(g_out, g_in.at[k], lat_s.at[k], lat_r.at[k], (lax.rem(band + k, n_lat), me))
        c.start()
        lat_copies.append(c)
        sent.append(c)

    for v in range(vp):
        sq, off, pr, sp = [tot[s * vp + v] * points for s in range(4)]
        tr = jnp.broadcast_to(tot[4 * vp + v // 4, v % 4:v % 4 + 1, :], (leads, lanes)) * points
        fin[me, v] = sq
        fin[me, vp + v] = off
        fin[me, 2 * vp + v] = pr / jnp.sqrt(jnp.maximum(sp, FLOOR) * jnp.maximum(tr, FLOOR))
    gather_z, gather_y = {}, {}
    if pair == 2:
        c = remote(fin.at[me], fin.at[me], agy_s.at[0], agy_r.at[0], partner)
        c.start()
        gather_y[0] = c
        sent.append(c)
    for k in range(1, outer):
        c = remote(fin.at[me], fin.at[me], agz_s.at[k], agz_r.at[k], (band, other(k) * pair + b))
        c.start()
        gather_z[k] = c
        sent.append(c)

    for c in lat_copies:
        c.wait_recv()
    gs = g_out[...]
    for k in range(1, n_lat):
        gs = gs + g_in[k]
    gs = gs / float(total_rows * cols * n_lon)
    g_mine[...] = gs
    g_all[me, 0:1, :] = jnp.sqrt(jnp.maximum(g_mine[0:1, :], FLOOR))
    g_all[me, 1:2, :] = g_mine[1:2, :]
    g_all[me, 2:3, :] = g_mine[2:3, :] / jnp.sqrt(
        jnp.maximum(g_mine[3:4, :], FLOOR) * jnp.maximum(g_mine[4:5, :], FLOOR))
    g_all[me, 3:8, :] = jnp.zeros((5, g_all.shape[2]), jnp.float32)
    lon_copies = []
    for k in range(1, n_lon):
        c = remote(g_all.at[me], g_all.at[me], lon_s.at[k], lon_r.at[k], (band, lax.rem(me + k, n_lon)))
        c.start()
        lon_copies.append(c)
        sent.append(c)

    for k in sorted(range(1, outer), key=lambda k: min(k, outer - k)):
        gather_z[k].wait_recv()
        if pair == 2:
            source = fin.at[lax.rem(a - k + outer, outer) * pair + b]
            c = remote(source, source, agy_s.at[k], agy_r.at[k], partner)
            c.start()
            gather_y[k] = c
            sent.append(c)
    for c in lon_copies:
        c.wait_recv()
    for d in range(n_lon):
        for l in range(leads):
            g_tmp[l, 0:3, starts[d]:starts[d] + vp] = g_all[d, 0:3, l * vp:(l + 1) * vp]
    for l in range(leads):
        for m, out in enumerate((g_rmse, g_off, g_skill)):
            out[l:l + 1, :] = g_tmp[l, m:m + 1, 0:nvars]
    for k in gather_y:
        gather_y[k].wait_recv()
    for d in range(n_lon):
        for m, out in enumerate((o_sq, o_off, o_skill)):
            out[starts[d]:starts[d] + vp] = fin[d, m * vp:(m + 1) * vp]
    for c in sent:
        c.wait_send()


def local(n_lat, n_lon, pred, ver, norm, flag, par):
    leads, nvars, cols, lanes = pred.shape
    vp = -(-nvars // n_lon)
    outer = n_lon // 2 if n_lon % 2 == 0 else n_lon
    blocks = 4 * vp + -(-vp // 4)
    glanes = -(-leads * vp // 128) * 128
    f32 = jnp.float32
    dma = pltpu.SemaphoreType.DMA
    vmem = pl.BlockSpec(memory_space=pltpu.VMEM)
    hbm = pl.BlockSpec(memory_space=pl.ANY)
    zonal = jax.ShapeDtypeStruct((nvars, leads, lanes), f32)
    whole = jax.ShapeDtypeStruct((leads, nvars), f32)
    out = pl.pallas_call(
        functools.partial(kernel, n_lat, n_lon, vp),
        out_shape=(zonal,) * 3 + (whole,) * 3,
        in_specs=[pl.BlockSpec(memory_space=pltpu.SMEM)] + [hbm] * 4,
        out_specs=(vmem,) * 6,
        scratch_shapes=[
            pltpu.VMEM((n_lon, vp, cols, leads, lanes), f32),
            pltpu.VMEM((cols, nvars, lanes), f32),
            pltpu.VMEM((cols, nvars, lanes), f32),
            pltpu.VMEM((cols, lanes), jnp.int32),
            pltpu.VMEM((cols, lanes), f32),
            pltpu.VMEM((nvars, lanes), f32),
            pltpu.VMEM((n_lon, blocks, 4, lanes), f32),
            pltpu.VMEM((outer, blocks, 4, lanes), f32),
            pltpu.VMEM((outer, blocks, 4, lanes), f32),
            pltpu.VMEM((outer, blocks, 4, lanes), f32),
            pltpu.VMEM((blocks, 4, lanes), f32),
            pltpu.VMEM((5, leads * vp, lanes), f32),
            pltpu.VMEM((n_lon, 3 * vp, leads, lanes), f32),
            pltpu.VMEM((8, glanes), f32),
            pltpu.VMEM((n_lat, 8, glanes), f32),
            pltpu.VMEM((8, glanes), f32),
            pltpu.VMEM((n_lon, 8, glanes), f32),
            pltpu.VMEM((leads, 8, 128 * (-(-nvars // 128))), f32),
            dma((3,)), dma((n_lon,)),
            dma((outer,)), dma((outer,)), dma((outer,)), dma((outer,)),
            dma((outer,)), dma((outer,)), dma((outer,)), dma((outer,)),
            dma((n_lat,)), dma((n_lat,)), dma((n_lon,)), dma((n_lon,)),
        ],
        compiler_params=pltpu.CompilerParams(collective_id=0, has_side_effects=True),
    )(par, jnp.transpose(pred, (1, 2, 0, 3)), jnp.transpose(ver, (1, 0, 2)), jnp.transpose(norm, (1, 0, 2)), flag)
    return tuple(jnp.transpose(x, (1, 0, 2)) for x in out[:3]) + tuple(out[3:])


def solution(mesh):
    n_lat, n_lon = mesh.shape["lat"], mesh.shape["lon"]
    in_specs = (
        P(None, None, "lon", "lat"),
        P(None, "lon", "lat"),
        P(None, "lon", "lat"),
        P("lon", "lat"),
        P(),
    )
    out_specs = (P(None, None, "lat"), P(None, None, "lat"), P(None, None, "lat"), P(), P(), P())
    return jax.shard_map(functools.partial(local, n_lat, n_lon), mesh=mesh, in_specs=in_specs, out_specs=out_specs,
                         check_vma=False)
```
